16 devices in a mesh: rep: 2 (over y, z), dp: 8 (over x, core).
Axes of the slice: x: 4, y: 2, z: 1, core: 2. Of those that a mesh axis runs over, the one named last changes fastest.
The devices are a block of a 4x4x8 slice.
Arguments:
- x: bfloat16 [16, 1024, 512], P(('rep', 'dp')), parts along dimension 0
- dy: bfloat16 [16, 1024, 512], P(('rep', 'dp')), parts along dimension 0
- wq: bfloat16 [2, 512, 2048], P(None, 'dp')
- wk: bfloat16 [2, 512, 2048], P(None, 'dp')
- wv: bfloat16 [2, 512, 2048], P(None, 'dp')
- wo: bfloat16 [2, 2048, 512], P(None, 'dp')
- w_gate: bfloat16 [2, 512, 8192], P(None, 'dp')
- w_up: bfloat16 [2, 512, 8192], P(None, 'dp')
- w_down: bfloat16 [2, 8192, 512], P(None, 'dp')
Outputs:
- output 1: bfloat16 [16, 1024, 512], P(('rep', 'dp')), parts along dimension 0
- output 2: bfloat16 [4, 512, 2048], P('rep', 'dp'), parts along dimension 0
- output 3: bfloat16 [4, 512, 2048], P('rep', 'dp'), parts along dimension 0
- output 4: bfloat16 [4, 512, 2048], P('rep', 'dp'), parts along dimension 0
- output 5: bfloat16 [4, 2048, 512], P('rep', 'dp'), parts along dimension 0
- output 6: bfloat16 [4, 512, 8192], P('rep', 'dp'), parts along dimension 0
- output 7: bfloat16 [4, 512, 8192], P('rep', 'dp'), parts along dimension 0
- output 8: bfloat16 [4, 8192, 512], P('rep', 'dp'), parts along dimension 0
There are 2 independent parts. The reference program is written for one: setup_inputs(seed, part) draws one part's arguments, and reference() takes and returns one part's arrays. A program takes and returns all parts, laid end to end along the dimension named above; an argument that names none is the same for every part.
All inputs are finite; a program needn't handle non-finite values.
Results may differ from the reference program's by a relative error of at most 0.0264.
Values are sent between devices in bfloat16 or wider.
A program may use at most 768 MiB of HBM per device.

```python
import jax
import jax.numpy as jnp
from jax import lax

SEQUENCES = 8
TOKENS = 1024
D = 512
HEADS = 16
KV_HEADS = 16
HEAD = 128
FF = 8192
LAYERS = 2
THETA = 10000
NAMES = ("wq", "wk", "wv", "wo", "w_gate", "w_up", "w_down")
SHAPES = {
    "wq": (LAYERS, D, HEADS * HEAD),
    "wk": (LAYERS, D, KV_HEADS * HEAD),
    "wv": (LAYERS, D, KV_HEADS * HEAD),
    "wo": (LAYERS, HEADS * HEAD, D),
    "w_gate": (LAYERS, D, FF),
    "w_up": (LAYERS, D, FF),
    "w_down": (LAYERS, FF, D),
}


def bump(key, n, height):
    away = (jnp.arange(n, dtype=jnp.int32) - jax.random.randint(key, (), 0, n, jnp.int32)) % n
    return jnp.where(away < n // 8, height, 1.0)


def together(key, own, strength):
    shared = jax.random.normal(key, own.shape[1:], jnp.float32)
    return (own + strength * shared) * lax.rsqrt(1 + strength * strength)


def setup_inputs(seed: int = 0, part: int = 0) -> dict:
    kx, kdy, ka, kb, kz, kf, kh, kl, *keys = jax.random.split(jax.random.key(seed), 8 + 3 * len(NAMES))
    kx, kdy, ka, kb = (jax.random.fold_in(k, part) for k in (kx, kdy, ka, kb))
    kw, km, kv = (keys[i::3] for i in range(3))
    shape = (SEQUENCES, TOKENS, D)
    much_x, much_dy = jax.random.uniform(kz, (2,), jnp.float32, 0.0, 1.0)
    loud = 2.0 ** jax.random.uniform(jax.random.fold_in(kz, 1), (), jnp.float32, -1.0, 2.0)
    layers = 2.0 ** jax.random.uniform(kl, (LAYERS, 1, 1), jnp.float32, -1.0, 1.0)
    times = {"wq": 1.0, "wk": 1.0, "wv": 2.0, "wo": layers, "w_gate": 1.0, "w_up": bump(kh, FF, 4.0), "w_down": layers}
    x = together(ka, jax.random.normal(kx, shape, jnp.float32), much_x) * bump(kf, D, 4.0)
    dy = together(kb, jax.random.normal(kdy, shape, jnp.float32), much_dy)
    drawn = {"x": x.astype(jnp.bfloat16), "dy": (loud * dy * (SEQUENCES * TOKENS) ** -0.5).astype(jnp.bfloat16)}
    for key, name in zip(kw, NAMES, strict=True):
        drawn[name] = (jax.random.normal(key, SHAPES[name], jnp.float32) * SHAPES[name][1] ** -0.5 * times[name]).astype(jnp.bfloat16)
    return drawn


def matmul(a, w):
    return jnp.dot(a, w, preferred_element_type=jnp.float32).astype(jnp.bfloat16)


def normed(h):
    wide = h.astype(jnp.float32)
    scale = lax.rsqrt(jnp.mean(wide**2, -1, keepdims=True) + 1e-6)
    return (wide * scale).astype(jnp.bfloat16)


def turned(t, theta):
    half = t.shape[-1] // 2
    angle = jnp.arange(t.shape[0], dtype=jnp.float32)[:, None] * theta ** (-jnp.arange(half, dtype=jnp.float32) / half)
    cos, sin = jnp.cos(angle)[:, None], jnp.sin(angle)[:, None]
    a, b = t[..., :half].astype(jnp.float32), t[..., half:].astype(jnp.float32)
    return jnp.concatenate([a * cos - b * sin, b * cos + a * sin], -1).astype(jnp.bfloat16)


def seen_by(q, k, v):
    tokens, kv = q.shape[0], k.shape[1]
    q = q.reshape(tokens, kv, -1, q.shape[-1])
    scores = jnp.einsum("tgsd,ugd->gstu", q.astype(jnp.float32), k.astype(jnp.float32)) * q.shape[-1] ** -0.5
    place = jnp.arange(tokens)
    weights = jax.nn.softmax(jnp.where(place[:, None] >= place, scores, -jnp.inf), -1).astype(jnp.bfloat16)
    return jnp.einsum("gstu,ugd->tgsd", weights.astype(jnp.float32), v.astype(jnp.float32)).astype(jnp.bfloat16).reshape(tokens, -1)


def layer(h, w):
    a = normed(h)
    q, k = (turned(matmul(a, w[name]).reshape(h.shape[0], -1, HEAD), THETA) for name in ("wq", "wk"))
    h = h + matmul(seen_by(q, k, matmul(a, w["wv"]).reshape(h.shape[0], -1, HEAD)), w["wo"])
    b = normed(h)
    gate = jnp.dot(b, w["w_gate"], preferred_element_type=jnp.float32)
    up = jnp.dot(b, w["w_up"], preferred_element_type=jnp.float32)
    return h + matmul((jax.nn.silu(gate) * up).astype(jnp.bfloat16), w["w_down"])


def stack(weights, h):
    return lax.scan(lambda h, w: (layer(h, w), None), h, weights)[0]


def reference(x, dy, wq, wk, wv, wo, w_gate, w_up, w_down):
    weights = dict(zip(NAMES, (wq, wk, wv, wo, w_gate, w_up, w_down), strict=True))

    def take(so_far, sequence):
        h, by_y = sequence
        _, back = jax.vjp(stack, weights, h)
        by_weights, by_h = back(by_y)
        return jax.tree.map(lambda total, term: total + term.astype(jnp.float32), so_far, by_weights), by_h

    none_yet = {name: jnp.zeros(w.shape, jnp.float32) for name, w in weights.items()}
    by_weights, by_x = lax.scan(take, none_yet, (x, dy))
    return (by_x, *(by_weights[name].astype(jnp.bfloat16) for name in NAMES))
```

```python
import functools

import jax
import jax.numpy as jnp
from jax import lax
from jax.experimental import pallas as pl
from jax.experimental.pallas import tpu as pltpu
from jax.sharding import PartitionSpec as P

HEAD = 128
THETA = 10000
EPS = 1e-6
LOG2E = 1.4426950408889634
HIDDEN = -2e30
VMEM = 60 * 2**20
BQ = 256
ANY = pl.BlockSpec(memory_space=pl.ANY)
low, wide = jnp.bfloat16, jnp.float32


def dot(a, b, ca=1, cb=0):
    return lax.dot_general(a, b, (((ca,), (cb,)), ((), ())), preferred_element_type=wide)


def inverse(h):
    return lax.rsqrt(jnp.mean(h * h, -1, keepdims=True) + EPS)


def normed(h):
    h = h.astype(wide)
    return (h * inverse(h)).astype(low)


def normed_back(by_out, h):
    h = h.astype(wide)
    s = inverse(h)
    return (by_out * s - h * (s * s * s * jnp.mean(by_out * h, -1, keepdims=True))).astype(low)


def plus(a, b):
    return (a.astype(wide) + b.astype(wide)).astype(low)


def turn(t, cos, sin):
    return (t * cos + pltpu.roll(t, HEAD // 2, 1) * sin).astype(low)


def tables(tokens):
    half = HEAD // 2
    angle = jnp.arange(tokens, dtype=wide)[:, None] * THETA ** (-jnp.arange(half, dtype=wide) / half)
    cos, sin = jnp.cos(angle), jnp.sin(angle)
    return jnp.concatenate([cos, cos], -1), jnp.concatenate([-sin, sin], -1)


def hide(s, first):
    size = s.shape[0] - first
    ok = lax.broadcasted_iota(jnp.int32, (size, s.shape[1]), 0) <= lax.broadcasted_iota(jnp.int32, (size, s.shape[1]), 1)
    part = jnp.where(ok, s[first:], HIDDEN)
    return part if first == 0 else jnp.concatenate([s[:first], part], axis=0)


def params(**more):
    return pltpu.CompilerParams(vmem_limit_bytes=VMEM, **more)


def attn_forward_kernel(h_ref, wq_ref, wk_ref, wv_ref, wo_ref, cos_ref, sin_ref, q_ref, k_ref, v_ref, o_ref, lse_ref, mid_ref, b_ref, a_s, acc_s):
    tokens, d = h_ref.shape
    step = pl.program_id(0)
    width = q_ref.shape[1]
    e = HEAD**-0.5 * LOG2E

    @pl.when(step == 0)
    def _():
        a_s[...] = normed(h_ref[...])
        acc_s[...] = jnp.zeros_like(acc_s)

    a = a_s[...]
    cos, sin = cos_ref[...], sin_ref[...]
    heads = [slice(i, i + HEAD) for i in range(0, width, HEAD)]
    for w_ref, out in ((wq_ref, q_ref), (wk_ref, k_ref)):
        t = dot(a, w_ref[...].reshape(d, width)).astype(low).astype(wide)
        for at in heads:
            out[:, at] = turn(t[:, at], cos, sin)
    v_ref[...] = dot(a, wv_ref[...].reshape(d, width)).astype(low)
    turned_v = [v_ref[:, at].T for at in heads]
    for first in range(0, tokens, BQ):
        last = first + BQ
        scores = [hide(dot(k_ref[:last, at], q_ref[first:last, at], 1, 1), first) for at in heads]
        for i, (at, s) in enumerate(zip(heads, scores)):
            top = s.max(axis=0, keepdims=True)
            p = jnp.exp2((s - top) * e)
            total = p.sum(axis=0, keepdims=True)
            out = dot(turned_v[i][:, :last], p.astype(low)) * (1 / total)
            o_ref[first:last, at] = out.T.astype(low)
            lse_ref[0, i : i + 1, first:last] = top * e + jnp.log2(total)
    acc_s[...] += dot(o_ref[...], wo_ref[0])

    @pl.when(step == pl.num_programs(0) - 1)
    def _():
        mid = plus(h_ref[...], acc_s[...].astype(low))
        mid_ref[...] = mid
        b_ref[...] = normed(mid)


def attn_specs(n, d, width, base):
    rows, per = d // n, d // width
    specs = [pl.BlockSpec((n, rows, width), lambda s, m=m: (0, base // rows + m * (n // per) + s // per, s % per)) for m in range(3)]
    tall = width
    return specs + [pl.BlockSpec((1, tall, d), lambda s: (s, (base + 3 * tall) // tall, 0))]


def attn_forward(h, packed, base, cos, sin, n, width):
    tokens, d = h.shape
    every = pl.BlockSpec((tokens, d), lambda s: (0, 0))
    table = pl.BlockSpec((tokens, HEAD), lambda s: (0, 0))
    part = pl.BlockSpec((tokens, width), lambda s: (0, s))
    heads = width // HEAD
    long = jax.ShapeDtypeStruct((tokens, n * width), low)
    short = jax.ShapeDtypeStruct((tokens, d), low)
    return pl.pallas_call(
        attn_forward_kernel,
        grid=(n,),
        in_specs=[every, *attn_specs(n, d, width, base), table, table],
        out_specs=[part] * 4 + [pl.BlockSpec((1, heads, tokens), lambda s: (s, 0, 0)), every, every],
        out_shape=[long] * 4 + [jax.ShapeDtypeStruct((n, heads, tokens), wide), short, short],
        scratch_shapes=[pltpu.VMEM((tokens, d), low), pltpu.VMEM((tokens, d), wide)],
        compiler_params=params(dimension_semantics=("arbitrary",)),
        cost_estimate=pl.CostEstimate(flops=n * width * tokens * (8 * d + 3 * tokens), transcendentals=n * heads * tokens * tokens // 2,
                                      bytes_accessed=8 * tokens * n * width + 8 * d * n * width),
        name="attn_forward",
    )(h, packed, packed, packed, packed, cos, sin)


def attn_back_kernel(by_ref, h_ref, q_ref, k_ref, v_ref, o_ref, lse_ref, wq_ref, wk_ref, wv_ref, wo_ref, cos_ref, sin_ref, *rest, base, aliased):
    by_h_ref, grads_ref, a_s, at_s, acc_s, dq_s, dk_s, dv_s, cols_s, rows_s, sems = rest[1:] if aliased else rest
    tokens, d = h_ref.shape
    step, steps = pl.program_id(0), pl.num_programs(0)
    slot = lax.rem(step, 2)
    n, rows = wq_ref.shape[0], wq_ref.shape[1]
    width = q_ref.shape[1]
    scale = HEAD**-0.5
    e = scale * LOG2E
    per = d // width

    def copies(s):
        k = lax.rem(s, 2)
        at = pl.multiple_of(lax.rem(s, per) * width, width)
        out = [pltpu.make_async_copy(cols_s.at[k, m], grads_ref.at[:, pl.ds(base + m * width + lax.div(s, per) * rows, rows), pl.ds(at, width)],
                                     sems.at[k, m]) for m in range(3)]
        return out + [pltpu.make_async_copy(rows_s.at[k], grads_ref.at[s, pl.ds(base + 3 * width, width), :], sems.at[k, 3])]

    @pl.when(step == 0)
    def _():
        a = normed(h_ref[...])
        at_s[...] = a.T
        acc_s[...] = jnp.zeros_like(acc_s)

    @pl.when(step >= 2)
    def _():
        for c in copies(step - 2):
            c.wait()

    by = by_ref[...]
    wo = wo_ref[0]
    by_o = dot(by, wo, 1, 1).astype(low)
    rows_s[slot] = dot(o_ref[...].T, by).astype(low)
    heads = [slice(i, i + HEAD) for i in range(0, width, HEAD)]
    count = len(heads)
    delta = [(by_o[:, at].astype(wide) * o_ref[:, at].astype(wide)).T.sum(axis=0, keepdims=True) for at in heads]
    turned_k = [k_ref[:, at].T for at in heads]
    for first in reversed(range(0, tokens, BQ)):
        last = first + BQ
        here = slice(first, last)
        scores = [dot(k_ref[:last, at], q_ref[here, at], 1, 1) for at in heads]
        by_p = [dot(v_ref[:last, at], by_o[here, at], 1, 1) for at in heads]
        for i, at in enumerate(heads):
            s = hide(scores[i] * e - lse_ref[0, i : i + 1, here], first)
            p = jnp.exp2(s)
            ds = (p * (by_p[i] - delta[i][:, here])).astype(low)
            p = p.astype(low)
            dv = dot(p, by_o[here, at])
            dk = dot(ds, q_ref[here, at])
            if last == tokens:
                dv_s[i], dk_s[i] = dv, dk
            else:
                dv_s[i, :last, :] += dv
                dk_s[i, :last, :] += dk
            dq_s[here, at] = (dot(turned_k[i][:, :last], ds) * scale).T.astype(low)
    cos, sin = cos_ref[...], -sin_ref[...]
    join = lambda parts: parts[0] if count == 1 else jnp.concatenate(parts, axis=1)
    dq = join([turn(dq_s[:, at].astype(wide), cos, sin) for at in heads])
    dk = join([turn((dk_s[i] * scale).astype(low).astype(wide), cos, sin) for i in range(count)])
    dv = join([dv_s[i].astype(low) for i in range(count)])
    at = at_s[...]
    total = None
    for m, (g, w_ref) in enumerate(((dq, wq_ref), (dk, wk_ref), (dv, wv_ref))):
        cols_s[slot, m] = dot(at, g).astype(low).reshape(n, rows, width)
        term = dot(g, w_ref[...].reshape(d, width), 1, 1)
        total = term if total is None else total + term
    acc_s[...] += total
    for c in copies(step):
        c.start()

    @pl.when(step == steps - 1)
    def _():
        by_a = acc_s[...].astype(low).astype(wide)
        by_h_ref[...] = plus(by, normed_back(by_a, h_ref[...]))
        for c in copies(step - 1) + copies(step):
            c.wait()


def attn_back(by, h, saved, packed, base, cos, sin, grads, n, width, grads_base):
    tokens, d = h.shape
    q, k, v, o, lse = saved
    aliased = isinstance(grads, jax.Array)
    every = pl.BlockSpec((tokens, d), lambda s: (0, 0))
    table = pl.BlockSpec((tokens, HEAD), lambda s: (0, 0))
    part = pl.BlockSpec((tokens, width), lambda s: (0, s))
    heads = width // HEAD
    rows = d // n
    given = [by, h, q, k, v, o, lse, packed, packed, packed, packed, cos, sin]
    specs = [every, every, part, part, part, part, pl.BlockSpec((1, heads, tokens), lambda s: (s, 0, 0)), *attn_specs(n, d, width, base), table, table]
    return pl.pallas_call(
        functools.partial(attn_back_kernel, base=grads_base, aliased=aliased),
        grid=(n,),
        in_specs=specs + [ANY] * aliased,
        out_specs=[every, ANY],
        out_shape=[jax.ShapeDtypeStruct((tokens, d), low), jax.ShapeDtypeStruct(grads.shape, low)],
        scratch_shapes=[pltpu.VMEM((tokens, d), low), pltpu.VMEM((d, tokens), low), pltpu.VMEM((tokens, d), wide), pltpu.VMEM((tokens, width), low),
                        pltpu.VMEM((heads, tokens, HEAD), wide), pltpu.VMEM((heads, tokens, HEAD), wide),
                        pltpu.VMEM((2, 3, n, rows, width), low), pltpu.VMEM((2, width, d), low), pltpu.SemaphoreType.DMA((2, 4))],
        input_output_aliases={len(given): 1} if aliased else {},
        compiler_params=params(dimension_semantics=("arbitrary",)),
        cost_estimate=pl.CostEstimate(flops=n * width * tokens * (16 * d + 7 * tokens), transcendentals=n * heads * tokens * tokens // 2,
                                      bytes_accessed=8 * tokens * n * width + 16 * d * n * width),
        name="attn_back",
    )(*given, *([grads] if aliased else []))


def ff_forward_kernel(b_ref, mid_ref, wg_ref, wu_ref, wd_ref, y_ref, acc_s):
    step = pl.program_id(0)
    d = b_ref.shape[1]
    b = b_ref[...]
    gate = dot(b, wg_ref[...].reshape(d, -1))
    up = dot(b, wu_ref[...].reshape(d, -1))
    hidden = (gate * jax.nn.sigmoid(gate) * up).astype(low)
    y = dot(hidden, wd_ref[0])

    @pl.when(step == 0)
    def _():
        acc_s[...] = y

    @pl.when(step > 0)
    def _():
        acc_s[...] += y

    @pl.when(step == pl.num_programs(0) - 1)
    def _():
        y_ref[...] = plus(mid_ref[...], acc_s[...].astype(low))


def ff_forward(b, mid, packed, base, n):
    tokens, d = b.shape
    rows = d // n
    half = 3 * d // rows
    every = pl.BlockSpec((tokens, d), lambda s: (0, 0))
    column = lambda m: pl.BlockSpec((n, rows, d), lambda s: (0, base // rows + s // n * half + m * n + s % n, 0))
    return pl.pallas_call(
        ff_forward_kernel,
        grid=(2 * n,),
        in_specs=[every, every, column(0), column(1), pl.BlockSpec((1, d, d), lambda s: (s % n, base // d + s // n * 3 + 2, 0))],
        out_specs=every,
        out_shape=jax.ShapeDtypeStruct((tokens, d), low),
        scratch_shapes=[pltpu.VMEM((tokens, d), wide)],
        compiler_params=params(dimension_semantics=("arbitrary",)),
        cost_estimate=pl.CostEstimate(flops=12 * n * tokens * d * d, transcendentals=2 * n * tokens * d, bytes_accessed=12 * n * d * d),
        name="ff_forward",
    )(b, mid, packed, packed, packed)


def ff_back_kernel(b_ref, by_ref, wg_ref, wu_ref, wd_ref, *rest, base, second, aliased):
    if second:
        acc_ref, mid_ref, *rest = rest
    if aliased:
        rest = rest[1:]
    by_ref_out, grads_ref, bt_s, acc_s, cols_s, rows_s, sems = rest
    step, steps = pl.program_id(0), pl.num_programs(0)
    slot = lax.rem(step, 2)
    n, rows, d = wg_ref.shape

    def copies(s):
        k = lax.rem(s, 2)
        out = [pltpu.make_async_copy(cols_s.at[k, m], grads_ref.at[:, pl.ds(base + m * d + s * rows, rows), :], sems.at[k, m]) for m in range(2)]
        return out + [pltpu.make_async_copy(rows_s.at[k], grads_ref.at[s, pl.ds(base + 2 * d, d), :], sems.at[k, 2])]

    @pl.when(step == 0)
    def _():
        bt_s[...] = b_ref[...].T
        acc_s[...] = acc_ref[...] if second else jnp.zeros_like(acc_s)

    @pl.when(step >= 2)
    def _():
        for c in copies(step - 2):
            c.wait()

    b, by, bt = b_ref[...], by_ref[...], bt_s[...]
    wg, wu, wd = wg_ref[...].reshape(d, d), wu_ref[...].reshape(d, d), wd_ref[0]
    gate, up = dot(b, wg), dot(b, wu)
    by_hidden = dot(by, wd, 1, 1).astype(low).astype(wide)
    sig = jax.nn.sigmoid(gate)
    silu = gate * sig
    hidden = (silu * up).astype(low)
    by_up = (by_hidden * silu).astype(low)
    by_gate = (by_hidden * up * (sig * (1 + gate * (1 - sig)))).astype(low)
    rows_s[slot] = dot(hidden.T, by).astype(low)
    cols_s[slot, 0] = dot(bt, by_gate).astype(low).reshape(n, rows, d)
    cols_s[slot, 1] = dot(bt, by_up).astype(low).reshape(n, rows, d)
    acc_s[...] += dot(by_gate, wg, 1, 1) + dot(by_up, wu, 1, 1)
    for c in copies(step):
        c.start()

    @pl.when(step == steps - 1)
    def _():
        if second:
            by_ref_out[...] = plus(by, normed_back(acc_s[...].astype(low).astype(wide), mid_ref[...]))
        else:
            by_ref_out[...] = acc_s[...]
        for c in copies(step - 1) + copies(step):
            c.wait()


def ff_back(b, by, packed, base, grads, n, grads_base, acc=None, mid=None):
    tokens, d = b.shape
    rows = d // n
    second = acc is not None
    aliased = isinstance(grads, jax.Array)
    every = pl.BlockSpec((tokens, d), lambda s: (0, 0))
    column = lambda m: pl.BlockSpec((n, rows, d), lambda s: (0, base // rows + m * n + s, 0))
    given = [b, by, packed, packed, packed] + ([acc, mid] if second else [])
    specs = [every, every, column(0), column(1), pl.BlockSpec((1, d, d), lambda s: (s, base // d + 2, 0))] + [every] * (2 * second)
    return pl.pallas_call(
        functools.partial(ff_back_kernel, base=grads_base, second=second, aliased=aliased),
        grid=(n,),
        in_specs=specs + [ANY] * aliased,
        out_specs=[every, ANY],
        out_shape=[jax.ShapeDtypeStruct((tokens, d), low if second else wide), jax.ShapeDtypeStruct(grads.shape, low)],
        scratch_shapes=[pltpu.VMEM((d, tokens), low), pltpu.VMEM((tokens, d), wide), pltpu.VMEM((2, 2, n, rows, d), low),
                        pltpu.VMEM((2, d, d), low), pltpu.SemaphoreType.DMA((2, 3))],
        input_output_aliases={len(given): 1} if aliased else {},
        compiler_params=params(dimension_semantics=("arbitrary",)),
        cost_estimate=pl.CostEstimate(flops=16 * n * tokens * d * d, transcendentals=n * tokens * d, bytes_accessed=12 * n * d * d),
        name="ff_back",
    )(*given, *([grads] if aliased else []))


def moves(part, weights):
    d = weights[3].shape[2]
    rows = weights[0].shape[1]
    out, at = [], 0
    if part == "attn":
        for m in range(3):
            for j in range(0, weights[m].shape[2], d):
                out.append((m, slice(0, rows), slice(j, j + d), slice(at, at + rows)))
                at += rows
        tall = weights[3].shape[1]
        return out + [(3, slice(0, tall), slice(0, d), slice(at, at + tall))], at + tall
    for m in (4, 5):
        for j in range(part * d, weights[m].shape[2], 2 * d):
            out.append((m, slice(0, rows), slice(j, j + d), slice(at, at + rows)))
            at += rows
    return out + [(6, slice(part * d, part * d + d), slice(0, d), slice(at, at + d))], at + d


def layout(parts, weights):
    out, at = [], 0
    for part, layer in parts:
        inner, size = moves(part, weights)
        out += [(layer, m, r, c, slice(to.start + at, to.stop + at)) for m, r, c, to in inner]
        at += size
    return out, at


def pack(buffers, weights):
    plans = [layout(parts, weights) for parts in buffers]
    used = sorted({(layer, m) for plan, _ in plans for layer, m, *_ in plan})
    d = weights[3].shape[2]

    def kernel(*refs):
        given = dict(zip(used, refs))
        for (plan, _), out in zip(plans, refs[len(used) :]):
            for layer, m, r, c, to in plan:
                out[to, :] = given[layer, m][0, r, c]

    return pl.pallas_call(
        kernel,
        grid=(1,),
        in_specs=[pl.BlockSpec((1, *weights[m].shape[1:]), lambda s, layer=layer: (layer, 0, 0)) for layer, m in used],
        out_specs=[pl.BlockSpec((size, d), lambda s: (0, 0)) for _, size in plans],
        out_shape=[jax.ShapeDtypeStruct((size, d), low) for _, size in plans],
        compiler_params=params(),
        name="pack",
    )(*(weights[m] for _, m in used))


def unpack(buffers, shards, weights):
    plans = [layout(parts, weights) for parts in buffers]

    def kernel(*refs):
        outs = refs[len(shards) :]
        for (plan, _), given in zip(plans, refs):
            for layer, m, r, c, to in plan:
                outs[m][layer, r, c] = given[to, :]

    whole = lambda a: pl.BlockSpec(a.shape, lambda s: (0,) * a.ndim)
    return pl.pallas_call(
        kernel,
        grid=(1,),
        in_specs=[whole(a) for a in shards],
        out_specs=[whole(w) for w in weights],
        out_shape=[jax.ShapeDtypeStruct(w.shape, low) for w in weights],
        compiler_params=params(),
        name="unpack",
    )(*shards)


def solution(mesh):
    n = mesh.shape["dp"]

    def gather(shard):
        return lax.all_gather(shard, "dp", axis=0, tiled=True).reshape(n, *shard.shape)

    def scatter(grads):
        return lax.psum_scatter(grads.reshape(-1, grads.shape[2]), "dp", scatter_dimension=0, tiled=True)

    def step(x, dy, *weights):
        h0, by = x[0], dy[0]
        tokens, d = h0.shape
        width = weights[0].shape[2] // n
        attn, half = 4 * width, 3 * d
        cos, sin = tables(tokens)

        sends = [[("attn", 0)], [(0, 0), (1, 0), ("attn", 1)], [(0, 1)], [(1, 1)]]
        (first,) = pack(sends[:1], weights)
        others = pack(sends[1:], weights)
        w_attn0, w_mixed, w_ff1a, w_ff1b = (gather(s) for s in (first, *others))

        *saved0, mid0, b0 = attn_forward(h0, w_attn0, 0, cos, sin, n, width)
        h1 = ff_forward(b0, mid0, w_mixed, 0, n)
        *saved1, mid1, b1 = attn_forward(h1, w_mixed, 2 * half, cos, sin, n, width)

        new = lambda size: jax.ShapeDtypeStruct((n, size, d), low)
        acc, g1 = ff_back(b1, by, w_ff1a, 0, new(half), n, 0)
        by, g2 = ff_back(b1, by, w_ff1b, 0, new(half), n, 0, acc, mid1)
        by, g3 = attn_back(by, h1, saved1, w_mixed, 2 * half, cos, sin, new(attn + half), n, width, 0)
        acc, g3 = ff_back(b0, by, w_mixed, 0, g3, n, attn)
        by, g4 = ff_back(b0, by, w_mixed, half, new(attn + half), n, attn, acc, mid0)
        by, g4 = attn_back(by, h0, saved0, w_attn0, 0, cos, sin, g4, n, width, 0)

        back = [[(0, 1)], [(1, 1)], [("attn", 1), (0, 0)], [("attn", 0), (1, 0)]]
        grads = unpack(back, [scatter(g) for g in (g1, g2, g3, g4)], weights)
        return (by[None], *grads)

    states, cut = P(("rep", "dp"), None, None), P(None, "dp", None)
    return jax.shard_map(
        step,
        mesh=mesh,
        in_specs=(states, states) + (cut,) * 7,
        out_specs=(states,) + (P("rep", "dp", None),) * 7,
        check_vma=False,
    )
```

```python
import functools

import jax
import jax.numpy as jnp
from jax import lax
from jax.experimental import pallas as pl
from jax.experimental.pallas import tpu as pltpu
from jax.sharding import PartitionSpec as P

HEAD = 128
THETA = 10000
EPS = 1e-6
LOG2E = 1.4426950408889634
HIDDEN = -2e30
VMEM = 60 * 2**20
BQ = 256
ANY = pl.BlockSpec(memory_space=pl.ANY)
low, wide = jnp.bfloat16, jnp.float32


def dot(a, b, ca=1, cb=0):
    return lax.dot_general(a, b, (((ca,), (cb,)), ((), ())), preferred_element_type=wide)


def inverse(h):
    return lax.rsqrt(jnp.mean(h * h, -1, keepdims=True) + EPS)


def normed(h):
    h = h.astype(wide)
    return (h * inverse(h)).astype(low)


def normed_back(by_out, h):
    h = h.astype(wide)
    s = inverse(h)
    return (by_out * s - h * (s * s * s * jnp.mean(by_out * h, -1, keepdims=True))).astype(low)


def plus(a, b):
    return (a.astype(wide) + b.astype(wide)).astype(low)


def turn(t, cos, sin):
    return (t * cos + pltpu.roll(t, HEAD // 2, 1) * sin).astype(low)


def tables(tokens):
    half = HEAD // 2
    angle = jnp.arange(tokens, dtype=wide)[:, None] * THETA ** (-jnp.arange(half, dtype=wide) / half)
    cos, sin = jnp.cos(angle), jnp.sin(angle)
    return jnp.concatenate([cos, cos], -1), jnp.concatenate([-sin, sin], -1)


def hide(s, first):
    size = s.shape[0] - first
    ok = lax.broadcasted_iota(jnp.int32, (size, s.shape[1]), 0) <= lax.broadcasted_iota(jnp.int32, (size, s.shape[1]), 1)
    part = jnp.where(ok, s[first:], HIDDEN)
    return part if first == 0 else jnp.concatenate([s[:first], part], axis=0)


def params(**more):
    return pltpu.CompilerParams(vmem_limit_bytes=VMEM, **more)


def attn_forward_kernel(h_ref, wq_ref, wk_ref, wv_ref, wo_ref, cos_ref, sin_ref, q_ref, k_ref, v_ref, o_ref, lse_ref, mid_ref, b_ref, a_s, acc_s):
    tokens, d = h_ref.shape
    step = pl.program_id(0)
    width = q_ref.shape[1]
    e = HEAD**-0.5 * LOG2E

    @pl.when(step == 0)
    def _():
        a_s[...] = normed(h_ref[...])
        acc_s[...] = jnp.zeros_like(acc_s)

    a = a_s[...]
    cos, sin = cos_ref[...], sin_ref[...]
    heads = [slice(i, i + HEAD) for i in range(0, width, HEAD)]
    for w_ref, out in ((wq_ref, q_ref), (wk_ref, k_ref)):
        t = dot(a, w_ref[...].reshape(d, width)).astype(low).astype(wide)
        for at in heads:
            out[:, at] = turn(t[:, at], cos, sin)
    v_ref[...] = dot(a, wv_ref[...].reshape(d, width)).astype(low)
    turned_v = [v_ref[:, at].T for at in heads]
    for first in range(0, tokens, BQ):
        last = first + BQ
        scores = [hide(dot(k_ref[:last, at], q_ref[first:last, at], 1, 1), first) for at in heads]
        for i, (at, s) in enumerate(zip(heads, scores)):
            top = s.max(axis=0, keepdims=True)
            p = jnp.exp2((s - top) * e)
            total = p.sum(axis=0, keepdims=True)
            out = dot(turned_v[i][:, :last], p.astype(low)) * (1 / total)
            o_ref[first:last, at] = out.T.astype(low)
            lse_ref[0, i : i + 1, first:last] = top * e + jnp.log2(total)
    acc_s[...] += dot(o_ref[...], wo_ref[0])

    @pl.when(step == pl.num_programs(0) - 1)
    def _():
        mid = plus(h_ref[...], acc_s[...].astype(low))
        mid_ref[...] = mid
        b_ref[...] = normed(mid)


def attn_specs(n, d, width, base):
    rows, per = d // n, d // width
    specs = [pl.BlockSpec((n, rows, width), lambda s, m=m: (0, base // rows + m * (n // per) + s // per, s % per)) for m in range(3)]
    tall = width
    return specs + [pl.BlockSpec((1, tall, d), lambda s: (s, (base + 3 * tall) // tall, 0))]


def attn_forward(h, packed, base, cos, sin, n, width):
    tokens, d = h.shape
    every = pl.BlockSpec((tokens, d), lambda s: (0, 0))
    table = pl.BlockSpec((tokens, HEAD), lambda s: (0, 0))
    part = pl.BlockSpec((tokens, width), lambda s: (0, s))
    heads = width // HEAD
    long = jax.ShapeDtypeStruct((tokens, n * width), low)
    short = jax.ShapeDtypeStruct((tokens, d), low)
    return pl.pallas_call(
        attn_forward_kernel,
        grid=(n,),
        in_specs=[every, *attn_specs(n, d, width, base), table, table],
        out_specs=[part] * 4 + [pl.BlockSpec((1, heads, tokens), lambda s: (s, 0, 0)), every, every],
        out_shape=[long] * 4 + [jax.ShapeDtypeStruct((n, heads, tokens), wide), short, short],
        scratch_shapes=[pltpu.VMEM((tokens, d), low), pltpu.VMEM((tokens, d), wide)],
        compiler_params=params(dimension_semantics=("arbitrary",)),
        cost_estimate=pl.CostEstimate(flops=n * width * tokens * (8 * d + 3 * tokens), transcendentals=n * heads * tokens * tokens // 2,
                                      bytes_accessed=8 * tokens * n * width + 8 * d * n * width),
        name="attn_forward",
    )(h, packed, packed, packed, packed, cos, sin)


def attn_back_kernel(by_ref, h_ref, q_ref, k_ref, v_ref, o_ref, lse_ref, wq_ref, wk_ref, wv_ref, wo_ref, cos_ref, sin_ref, *rest, base, aliased):
    by_h_ref, grads_ref, a_s, at_s, acc_s, dq_s, dk_s, dv_s, cols_s, rows_s, sems = rest[1:] if aliased else rest
    tokens, d = h_ref.shape
    step, steps = pl.program_id(0), pl.num_programs(0)
    slot = lax.rem(step, 2)
    n, rows = wq_ref.shape[0], wq_ref.shape[1]
    width = q_ref.shape[1]
    scale = HEAD**-0.5
    e = scale * LOG2E
    per = d // width

    def copies(s):
        k = lax.rem(s, 2)
        at = pl.multiple_of(lax.rem(s, per) * width, width)
        out = [pltpu.make_async_copy(cols_s.at[k, m], grads_ref.at[:, pl.ds(base + m * width + lax.div(s, per) * rows, rows), pl.ds(at, width)],
                                     sems.at[k, m]) for m in range(3)]
        return out + [pltpu.make_async_copy(rows_s.at[k], grads_ref.at[s, pl.ds(base + 3 * width, width), :], sems.at[k, 3])]

    @pl.when(step == 0)
    def _():
        a = normed(h_ref[...])
        at_s[...] = a.T
        acc_s[...] = jnp.zeros_like(acc_s)

    @pl.when(step >= 2)
    def _():
        for c in copies(step - 2):
            c.wait()

    by = by_ref[...]
    wo = wo_ref[0]
    by_o = dot(by, wo, 1, 1).astype(low)
    rows_s[slot] = dot(o_ref[...].T, by).astype(low)
    heads = [slice(i, i + HEAD) for i in range(0, width, HEAD)]
    count = len(heads)
    delta = [(by_o[:, at].astype(wide) * o_ref[:, at].astype(wide)).T.sum(axis=0, keepdims=True) for at in heads]
    turned_k = [k_ref[:, at].T for at in heads]
    for first in reversed(range(0, tokens, BQ)):
        last = first + BQ
        here = slice(first, last)
        scores = [dot(k_ref[:last, at], q_ref[here, at], 1, 1) for at in heads]
        by_p = [dot(v_ref[:last, at], by_o[here, at], 1, 1) for at in heads]
        for i, at in enumerate(heads):
            s = hide(scores[i] * e - lse_ref[0, i : i + 1, here], first)
            p = jnp.exp2(s)
            ds = (p * (by_p[i] - delta[i][:, here])).astype(low)
            p = p.astype(low)
            dv = dot(p, by_o[here, at])
            dk = dot(ds, q_ref[here, at])
            if last == tokens:
                dv_s[i], dk_s[i] = dv, dk
            else:
                dv_s[i, :last, :] += dv
                dk_s[i, :last, :] += dk
            dq_s[here, at] = (dot(turned_k[i][:, :last], ds) * scale).T.astype(low)
    cos, sin = cos_ref[...], -sin_ref[...]
    join = lambda parts: parts[0] if count == 1 else jnp.concatenate(parts, axis=1)
    dq = join([turn(dq_s[:, at].astype(wide), cos, sin) for at in heads])
    dk = join([turn((dk_s[i] * scale).astype(low).astype(wide), cos, sin) for i in range(count)])
    dv = join([dv_s[i].astype(low) for i in range(count)])
    at = at_s[...]
    total = None
    for m, (g, w_ref) in enumerate(((dq, wq_ref), (dk, wk_ref), (dv, wv_ref))):
        cols_s[slot, m] = dot(at, g).astype(low).reshape(n, rows, width)
        term = dot(g, w_ref[...].reshape(d, width), 1, 1)
        total = term if total is None else total + term
    acc_s[...] += total
    for c in copies(step):
        c.start()

    @pl.when(step == steps - 1)
    def _():
        by_a = acc_s[...].astype(low).astype(wide)
        by_h_ref[...] = plus(by, normed_back(by_a, h_ref[...]))
        for c in copies(step - 1) + copies(step):
            c.wait()


def attn_back(by, h, saved, packed, base, cos, sin, grads, n, width, grads_base):
    tokens, d = h.shape
    q, k, v, o, lse = saved
    aliased = isinstance(grads, jax.Array)
    every = pl.BlockSpec((tokens, d), lambda s: (0, 0))
    table = pl.BlockSpec((tokens, HEAD), lambda s: (0, 0))
    part = pl.BlockSpec((tokens, width), lambda s: (0, s))
    heads = width // HEAD
    rows = d // n
    given = [by, h, q, k, v, o, lse, packed, packed, packed, packed, cos, sin]
    specs = [every, every, part, part, part, part, pl.BlockSpec((1, heads, tokens), lambda s: (s, 0, 0)), *attn_specs(n, d, width, base), table, table]
    return pl.pallas_call(
        functools.partial(attn_back_kernel, base=grads_base, aliased=aliased),
        grid=(n,),
        in_specs=specs + [ANY] * aliased,
        out_specs=[every, ANY],
        out_shape=[jax.ShapeDtypeStruct((tokens, d), low), jax.ShapeDtypeStruct(grads.shape, low)],
        scratch_shapes=[pltpu.VMEM((tokens, d), low), pltpu.VMEM((d, tokens), low), pltpu.VMEM((tokens, d), wide), pltpu.VMEM((tokens, width), low),
                        pltpu.VMEM((heads, tokens, HEAD), wide), pltpu.VMEM((heads, tokens, HEAD), wide),
                        pltpu.VMEM((2, 3, n, rows, width), low), pltpu.VMEM((2, width, d), low), pltpu.SemaphoreType.DMA((2, 4))],
        input_output_aliases={len(given): 1} if aliased else {},
        compiler_params=params(dimension_semantics=("arbitrary",)),
        cost_estimate=pl.CostEstimate(flops=n * width * tokens * (16 * d + 7 * tokens), transcendentals=n * heads * tokens * tokens // 2,
                                      bytes_accessed=8 * tokens * n * width + 16 * d * n * width),
        name="attn_back",
    )(*given, *([grads] if aliased else []))


def ff_forward_kernel(b_ref, mid_ref, wg_ref, wu_ref, wd_ref, y_ref, acc_s):
    step = pl.program_id(0)
    d = b_ref.shape[1]
    b = b_ref[...]
    gate = dot(b, wg_ref[...].reshape(d, -1))
    up = dot(b, wu_ref[...].reshape(d, -1))
    hidden = (gate * jax.nn.sigmoid(gate) * up).astype(low)
    y = dot(hidden, wd_ref[0])

    @pl.when(step == 0)
    def _():
        acc_s[...] = y

    @pl.when(step > 0)
    def _():
        acc_s[...] += y

    @pl.when(step == pl.num_programs(0) - 1)
    def _():
        y_ref[...] = plus(mid_ref[...], acc_s[...].astype(low))


def ff_forward(b, mid, packed, base, n):
    tokens, d = b.shape
    rows = d // n
    half = 3 * d // rows
    every = pl.BlockSpec((tokens, d), lambda s: (0, 0))
    column = lambda m: pl.BlockSpec((n, rows, d), lambda s: (0, base // rows + s // n * half + m * n + s % n, 0))
    return pl.pallas_call(
        ff_forward_kernel,
        grid=(2 * n,),
        in_specs=[every, every, column(0), column(1), pl.BlockSpec((1, d, d), lambda s: (s % n, base // d + s // n * 3 + 2, 0))],
        out_specs=every,
        out_shape=jax.ShapeDtypeStruct((tokens, d), low),
        scratch_shapes=[pltpu.VMEM((tokens, d), wide)],
        compiler_params=params(dimension_semantics=("arbitrary",)),
        cost_estimate=pl.CostEstimate(flops=12 * n * tokens * d * d, transcendentals=2 * n * tokens * d, bytes_accessed=12 * n * d * d),
        name="ff_forward",
    )(b, mid, packed, packed, packed)


def ff_back_kernel(b_ref, by_ref, wg_ref, wu_ref, wd_ref, *rest, base, second, aliased):
    if second:
        acc_ref, mid_ref, *rest = rest
    if aliased:
        rest = rest[1:]
    by_ref_out, grads_ref, bt_s, acc_s, cols_s, rows_s, sems = rest
    step, steps = pl.program_id(0), pl.num_programs(0)
    slot = lax.rem(step, 2)
    n, rows, d = wg_ref.shape

    def copies(s):
        k = lax.rem(s, 2)
        out = [pltpu.make_async_copy(cols_s.at[k, m], grads_ref.at[:, pl.ds(base + m * d + s * rows, rows), :], sems.at[k, m]) for m in range(2)]
        return out + [pltpu.make_async_copy(rows_s.at[k], grads_ref.at[s, pl.ds(base + 2 * d, d), :], sems.at[k, 2])]

    @pl.when(step == 0)
    def _():
        bt_s[...] = b_ref[...].T
        acc_s[...] = acc_ref[...] if second else jnp.zeros_like(acc_s)

    @pl.when(step >= 2)
    def _():
        for c in copies(step - 2):
            c.wait()

    b, by, bt = b_ref[...], by_ref[...], bt_s[...]
    wg, wu, wd = wg_ref[...].reshape(d, d), wu_ref[...].reshape(d, d), wd_ref[0]
    gate, up = dot(b, wg), dot(b, wu)
    by_hidden = dot(by, wd, 1, 1).astype(low).astype(wide)
    sig = jax.nn.sigmoid(gate)
    silu = gate * sig
    hidden = (silu * up).astype(low)
    by_up = (by_hidden * silu).astype(low)
    by_gate = (by_hidden * up * (sig * (1 + gate * (1 - sig)))).astype(low)
    rows_s[slot] = dot(hidden.T, by).astype(low)
    cols_s[slot, 0] = dot(bt, by_gate).astype(low).reshape(n, rows, d)
    cols_s[slot, 1] = dot(bt, by_up).astype(low).reshape(n, rows, d)
    acc_s[...] += dot(by_gate, wg, 1, 1) + dot(by_up, wu, 1, 1)
    for c in copies(step):
        c.start()

    @pl.when(step == steps - 1)
    def _():
        if second:
            by_ref_out[...] = plus(by, normed_back(acc_s[...].astype(low).astype(wide), mid_ref[...]))
        else:
            by_ref_out[...] = acc_s[...]
        for c in copies(step - 1) + copies(step):
            c.wait()


def ff_back(b, by, packed, base, grads, n, grads_base, acc=None, mid=None):
    tokens, d = b.shape
    rows = d // n
    second = acc is not None
    aliased = isinstance(grads, jax.Array)
    every = pl.BlockSpec((tokens, d), lambda s: (0, 0))
    column = lambda m: pl.BlockSpec((n, rows, d), lambda s: (0, base // rows + m * n + s, 0))
    given = [b, by, packed, packed, packed] + ([acc, mid] if second else [])
    specs = [every, every, column(0), column(1), pl.BlockSpec((1, d, d), lambda s: (s, base // d + 2, 0))] + [every] * (2 * second)
    return pl.pallas_call(
        functools.partial(ff_back_kernel, base=grads_base, second=second, aliased=aliased),
        grid=(n,),
        in_specs=specs + [ANY] * aliased,
        out_specs=[every, ANY],
        out_shape=[jax.ShapeDtypeStruct((tokens, d), low if second else wide), jax.ShapeDtypeStruct(grads.shape, low)],
        scratch_shapes=[pltpu.VMEM((d, tokens), low), pltpu.VMEM((tokens, d), wide), pltpu.VMEM((2, 2, n, rows, d), low),
                        pltpu.VMEM((2, d, d), low), pltpu.SemaphoreType.DMA((2, 3))],
        input_output_aliases={len(given): 1} if aliased else {},
        compiler_params=params(dimension_semantics=("arbitrary",)),
        cost_estimate=pl.CostEstimate(flops=16 * n * tokens * d * d, transcendentals=n * tokens * d, bytes_accessed=12 * n * d * d),
        name="ff_back",
    )(*given, *([grads] if aliased else []))


def places(n):
    me = lax.axis_index("dp")
    chip, core, chips = lax.div(me, 2), lax.rem(me, 2), n // 2
    return me, chip, core, [lax.rem(chip + hop, chips) for hop in (1, chips - 1, 2)], me + 1 - 2 * core


def meet(*others):
    barrier = pltpu.get_barrier_semaphore()
    for other in others:
        pl.semaphore_signal(barrier, inc=1, device_id={"dp": other}, device_id_type=pl.DeviceIdType.MESH)
    pl.semaphore_wait(barrier, len(others))


def gather_kernel(x_ref, *rest, n, pieces):
    out_ref, send, recv, local = rest[-4:]
    me, _, core, (right, left, far), partner = places(n)
    right, left, far = (2 * c + core for c in (right, left, far))
    size = x_ref.shape[0] // pieces
    meet(right, left, partner)

    def copy(kind, g, origin, to):
        rows = pl.ds(g * size, size)
        dst = out_ref.at[origin, rows, :]
        return pltpu.make_async_remote_copy(src_ref=x_ref.at[rows, :] if kind < 3 else dst, dst_ref=dst, send_sem=send.at[kind, g],
                                            recv_sem=recv.at[kind, g], device_id={"dp": to}, device_id_type=pl.DeviceIdType.MESH)

    own = pltpu.make_async_copy(x_ref, out_ref.at[me], local)
    own.start()
    copies = {}

    def go(kind, g, origin, to):
        copies[kind, g] = copy(kind, g, origin, to)
        copies[kind, g].start()

    for g in range(pieces):
        go(0, g, me, right)
        go(1, g, me, left)
    for g in range(pieces):
        go(2, g, me, partner)
    for g in range(pieces):
        copies[0, g].wait_recv()
        go(3, g, left, partner)
        if g % 2 == 0:
            go(5, g, left, right)
        copies[1, g].wait_recv()
        go(4, g, right, partner)
        if g % 2 == 1:
            go(5, g, right, left)
    for g in range(pieces):
        copies[5, g].wait_recv()
        go(6, g, far, partner)
    for g in range(pieces):
        for kind in (2, 3, 4, 6):
            copies[kind, g].wait_recv()
    for c in copies.values():
        c.wait_send()
    own.wait()


def gather_now(shard, n, call, after=None, pieces=4):
    more = [] if after is None else [after]
    return pl.pallas_call(
        functools.partial(gather_kernel, n=n, pieces=pieces),
        in_specs=[pl.BlockSpec(memory_space=pltpu.VMEM)] + [ANY] * len(more),
        out_specs=ANY,
        out_shape=jax.ShapeDtypeStruct((n, *shard.shape), shard.dtype),
        scratch_shapes=[pltpu.SemaphoreType.DMA((7, pieces)), pltpu.SemaphoreType.DMA((7, pieces)), pltpu.SemaphoreType.DMA],
        compiler_params=params(collective_id=call, has_side_effects=True),
        cost_estimate=pl.CostEstimate(flops=40 * 10**9, transcendentals=0, bytes_accessed=n * shard.size * 2),
        name="gather_now",
    )(shard, *more)


def scatter_kernel(x_ref, out_ref, pair_s, sum_s, far_s, near_s, send, recv, *, n, pieces):
    me, chip, core, (right, left, far), partner = places(n)
    chips, _, total, _ = x_ref.shape
    size = total // pieces
    other = 1 - core
    on_right, on_left = 2 * right + core, 2 * left + core
    meet(on_right, on_left, partner)
    at = [pl.ds(g * size, size) for g in range(pieces)]

    def copy(kind, g, src, dst, to):
        c = pltpu.make_async_remote_copy(src_ref=src, dst_ref=dst, send_sem=send.at[kind, g], recv_sem=recv.at[kind, g], device_id={"dp": to},
                                         device_id_type=pl.DeviceIdType.MESH)
        c.start()
        return c

    first = [copy(0, g, x_ref.at[:, other, at[g], :], pair_s.at[:, at[g], :], partner) for g in range(pieces)]
    second, third = [], []
    for g in range(pieces):
        first[g].wait_recv()
        for c in range(chips):
            sum_s[c, at[g], :] = plus(x_ref[c, core, at[g], :], pair_s[c, at[g], :])
        second.append(copy(1, g, sum_s.at[far, at[g], :], far_s.at[at[g], :], on_left if g % 2 else on_right))
    for g in range(pieces):
        second[g].wait_recv()
        towards = left if g % 2 else right
        sum_s[towards, at[g], :] = plus(sum_s[towards, at[g], :], far_s[at[g], :])
        third.append((copy(2, g, sum_s.at[right, at[g], :], near_s.at[0, at[g], :], on_right),
                      copy(3, g, sum_s.at[left, at[g], :], near_s.at[1, at[g], :], on_left)))
    for g in range(pieces):
        for c in third[g]:
            c.wait_recv()
        out_ref[at[g], :] = (sum_s[chip, at[g], :].astype(wide) + near_s[0, at[g], :].astype(wide) + near_s[1, at[g], :].astype(wide)).astype(low)
    for g in range(pieces):
        for c in (first[g], second[g], *third[g]):
            c.wait_send()


def scatter_now(grads, n, call, pieces=4):
    _, rows, d = grads.shape
    chips = n // 2
    return pl.pallas_call(
        functools.partial(scatter_kernel, n=n, pieces=pieces),
        in_specs=[pl.BlockSpec(memory_space=pltpu.VMEM)],
        out_specs=pl.BlockSpec(memory_space=pltpu.VMEM),
        out_shape=jax.ShapeDtypeStruct((rows, d), low),
        scratch_shapes=[pltpu.VMEM((chips, rows, d), low), pltpu.VMEM((chips, rows, d), low), pltpu.VMEM((rows, d), low), pltpu.VMEM((2, rows, d), low),
                        pltpu.SemaphoreType.DMA((4, pieces)), pltpu.SemaphoreType.DMA((4, pieces))],
        compiler_params=params(collective_id=call, has_side_effects=True),
        cost_estimate=pl.CostEstimate(flops=40 * 10**9, transcendentals=0, bytes_accessed=grads.size * 2),
        name="scatter_now",
    )(grads.reshape(chips, 2, rows, d))


def moves(part, weights):
    d = weights[3].shape[2]
    rows = weights[0].shape[1]
    out, at = [], 0
    if part == "attn":
        for m in range(3):
            for j in range(0, weights[m].shape[2], d):
                out.append((m, slice(0, rows), slice(j, j + d), slice(at, at + rows)))
                at += rows
        tall = weights[3].shape[1]
        return out + [(3, slice(0, tall), slice(0, d), slice(at, at + tall))], at + tall
    for m in (4, 5):
        for j in range(part * d, weights[m].shape[2], 2 * d):
            out.append((m, slice(0, rows), slice(j, j + d), slice(at, at + rows)))
            at += rows
    return out + [(6, slice(part * d, part * d + d), slice(0, d), slice(at, at + d))], at + d


def layout(parts, weights):
    out, at = [], 0
    for part, layer in parts:
        inner, size = moves(part, weights)
        out += [(layer, m, r, c, slice(to.start + at, to.stop + at)) for m, r, c, to in inner]
        at += size
    return out, at


def pack(buffers, weights):
    plans = [layout(parts, weights) for parts in buffers]
    used = sorted({(layer, m) for plan, _ in plans for layer, m, *_ in plan})
    d = weights[3].shape[2]

    def kernel(*refs):
        given = dict(zip(used, refs))
        for (plan, _), out in zip(plans, refs[len(used) :]):
            for layer, m, r, c, to in plan:
                out[to, :] = given[layer, m][0, r, c]

    return pl.pallas_call(
        kernel,
        grid=(1,),
        in_specs=[pl.BlockSpec((1, *weights[m].shape[1:]), lambda s, layer=layer: (layer, 0, 0)) for layer, m in used],
        out_specs=[pl.BlockSpec((size, d), lambda s: (0, 0)) for _, size in plans],
        out_shape=[jax.ShapeDtypeStruct((size, d), low) for _, size in plans],
        compiler_params=params(),
        name="pack",
    )(*(weights[m] for _, m in used))


def unpack(buffers, shards, weights, begun=None):
    plans = [layout(parts, weights) for parts in buffers]
    count = len(shards)

    def kernel(*refs):
        outs, sem = refs[-1 - len(weights) : -1], refs[-1]
        copies = [pltpu.make_async_copy(given.at[to, :], outs[m].at[layer, r, c], sem)
                  for (plan, _), given in zip(plans, refs) for layer, m, r, c, to in plan]
        for c in copies:
            c.start()
        for c in copies:
            c.wait()

    more = [] if begun is None else list(begun)
    return pl.pallas_call(
        kernel,
        in_specs=[pl.BlockSpec(memory_space=pltpu.VMEM)] * count + [ANY] * len(more),
        out_specs=[ANY] * len(weights),
        out_shape=[jax.ShapeDtypeStruct(w.shape, low) for w in weights],
        scratch_shapes=[pltpu.SemaphoreType.DMA],
        input_output_aliases={count + i: i for i in range(len(more))},
        compiler_params=params(),
        name="unpack",
    )(*shards, *more)


def solution(mesh):
    n = mesh.shape["dp"]

    def gather(shard):
        return lax.all_gather(shard, "dp", axis=0, tiled=True).reshape(n, *shard.shape)

    def scatter(grads):
        return lax.psum_scatter(grads.reshape(-1, grads.shape[2]), "dp", scatter_dimension=0, tiled=True)

    def step(x, dy, *weights):
        h0, by = x[0], dy[0]
        tokens, d = h0.shape
        width = weights[0].shape[2] // n
        attn, half = 4 * width, 3 * d
        cos, sin = tables(tokens)

        (s_attn0, s_ff0) = pack([[("attn", 0)], [(0, 0), (1, 0)]], weights)
        w_ff0 = gather(s_ff0)
        w_attn0 = gather_now(s_attn0, n, 0)
        s_attn1, s_ff1a, s_ff1b = pack([[("attn", 1)], [(0, 1)], [(1, 1)]], weights)
        w_ff1a, w_ff1b = gather(s_ff1a), gather(s_ff1b)

        *saved0, mid0, b0 = attn_forward(h0, w_attn0, 0, cos, sin, n, width)
        w_attn1 = gather_now(s_attn1, n, 1, after=b0)
        h1 = ff_forward(b0, mid0, w_ff0, 0, n)
        *saved1, mid1, b1 = attn_forward(h1, w_attn1, 0, cos, sin, n, width)

        new = lambda size: jax.ShapeDtypeStruct((n, size, d), low)
        acc, g1 = ff_back(b1, by, w_ff1a, 0, new(half), n, 0)
        by, g2 = ff_back(b1, by, w_ff1b, 0, new(half), n, 0, acc, mid1)
        by, g3 = attn_back(by, h1, saved1, w_attn1, 0, cos, sin, new(attn + half), n, width, 0)
        acc, g3 = ff_back(b0, by, w_ff0, 0, g3, n, attn)
        by, g4 = ff_back(b0, by, w_ff0, half, new(half), n, 0, acc, mid0)
        by, g5 = attn_back(by, h0, saved0, w_attn0, 0, cos, sin, new(attn), n, width, 0)

        m5 = scatter_now(g5, n, 2)
        m1, m2, m3, m4 = (scatter(g) for g in (g1, g2, g3, g4))
        grads = unpack([[(0, 1)], [(1, 1)], [("attn", 1), (0, 0)]], [m1, m2, m3], weights)
        grads = unpack([[(1, 0)], [("attn", 0)]], [m4, m5], weights, grads)
        return (by[None], *grads)

    states, cut = P(("rep", "dp"), None, None), P(None, "dp", None)
    return jax.shard_map(
        step,
        mesh=mesh,
        in_specs=(states, states) + (cut,) * 7,
        out_specs=(states,) + (P("rep", "dp", None),) * 7,
        check_vma=False,
    )
```
